32 devices in a mesh: ep: 32 (over z, y, x, core).
Axes of the slice: x: 2, y: 2, z: 4, core: 2. Of those that a mesh axis runs over, the one named last changes fastest.
Arguments:
- hidden: bfloat16 [16384, 1280], P('ep')
- w_router: float32 [1280, 32], replicated
- expert_ids: int32 [16384, 2], P('ep')
- w_one: bfloat16 [32, 1280, 5120], P('ep')
- w_three: bfloat16 [32, 1280, 5120], P('ep')
- w_two: bfloat16 [32, 5120, 1280], P('ep')
Outputs:
- output: bfloat16 [16384, 1280], P('ep')
All inputs are finite; a program needn't handle non-finite values.
Results may differ from the reference program's by a relative error of at most 0.00867312.
Values are sent between devices in bfloat16 or wider.
A program may use at most 1 GiB of HBM per device.

```python
import jax
import jax.numpy as jnp
from jax import lax

TOK_DEV = 512
GROUP = 32
D = 1280
FF = 5120
EXPERTS = 32
ROW_BLOCK = 32


def route_ids(key):
    key_hot, key_src = jax.random.split(key)
    dev_order = jax.random.permutation(key_hot, GROUP)
    n_hot = GROUP // 4
    n_cold = GROUP - n_hot
    row_cap = 4 * TOK_DEV // GROUP
    per_dev = EXPERTS // GROUP
    hot_devs = dev_order[:n_hot]
    cold_devs = dev_order[n_hot:]
    slot_idx = jnp.arange(TOK_DEV)

    def one_source(src_key):
        key_shift, key_first, key_second, key_flip, key_perm = jax.random.split(src_key, 5)
        shift_val = jax.random.randint(key_shift, (), 0, n_cold)
        first_dev = hot_devs[slot_idx // row_cap]
        second_dev = cold_devs[(slot_idx + shift_val) % n_cold]
        first_exp = first_dev * per_dev + jax.random.randint(key_first, (TOK_DEV,), 0, per_dev)
        second_exp = second_dev * per_dev + jax.random.randint(key_second, (TOK_DEV,), 0, per_dev)
        pair_ids = jnp.stack([first_exp, second_exp], axis=1)
        flip_bit = jax.random.randint(key_flip, (TOK_DEV, 1), 0, 2)
        pair_ids = jnp.where(flip_bit == 1, pair_ids[:, ::-1], pair_ids)
        token_perm = jax.random.permutation(key_perm, TOK_DEV)
        return pair_ids[token_perm]

    src_keys = jax.random.split(key_src, GROUP)
    return jax.vmap(one_source)(src_keys).reshape(GROUP * TOK_DEV, 2).astype(jnp.int32)


def setup_inputs(seed: int = 0) -> dict:
    key = jax.random.key(seed)
    key_hidden, key_router, key_ids, key_one, key_three, key_two = jax.random.split(key, 6)
    tok_count = GROUP * TOK_DEV
    hidden = jax.random.normal(key_hidden, (tok_count, D), jnp.float32).astype(jnp.bfloat16)
    w_router = jax.random.normal(key_router, (D, EXPERTS), jnp.float32) * D ** -0.5
    expert_ids = route_ids(key_ids)
    w_one = (jax.random.normal(key_one, (EXPERTS, D, FF), jnp.float32) * D ** -0.5).astype(jnp.bfloat16)
    w_three = (jax.random.normal(key_three, (EXPERTS, D, FF), jnp.float32) * D ** -0.5).astype(jnp.bfloat16)
    w_two = (jax.random.normal(key_two, (EXPERTS, FF, D), jnp.float32) * FF ** -0.5).astype(jnp.bfloat16)
    return {"hidden": hidden, "w_router": w_router, "expert_ids": expert_ids, "w_one": w_one, "w_three": w_three, "w_two": w_two}


def reference(hidden, w_router, expert_ids, w_one, w_three, w_two):
    tok_count = hidden.shape[0]
    model_dim = hidden.shape[1]
    logits = jnp.dot(hidden.astype(jnp.float32), w_router, preferred_element_type=jnp.float32)
    prob_vals = jax.nn.softmax(logits, axis=-1)
    picked = jnp.take_along_axis(prob_vals, expert_ids, axis=1)
    gate_vals = picked / jnp.sum(picked, axis=1, keepdims=True)
    flat_ids = expert_ids.reshape(-1)
    assign_count = flat_ids.shape[0]
    sort_order = jnp.argsort(flat_ids, stable=True)
    sorted_ids = flat_ids[sort_order]
    counts = jnp.zeros((EXPERTS,), jnp.int32).at[flat_ids].add(1)
    padded = (counts + ROW_BLOCK - 1) // ROW_BLOCK * ROW_BLOCK
    pad_end = jnp.cumsum(padded)
    pad_start = pad_end - padded
    first_row = jnp.cumsum(counts) - counts
    rank_in = jnp.arange(assign_count) - first_row[sorted_ids]
    dest_row = pad_start[sorted_ids] + rank_in
    row_total = assign_count + EXPERTS * ROW_BLOCK
    block_count = row_total // ROW_BLOCK
    row_tok = jnp.zeros((row_total,), jnp.int32).at[dest_row].set((sort_order // 2).astype(jnp.int32))
    block_start = jnp.arange(block_count) * ROW_BLOCK
    block_exp = jnp.minimum(jnp.sum((block_start[:, None] >= pad_end[None, :]).astype(jnp.int32), axis=1), EXPERTS - 1)
    hidden_blocks = hidden[row_tok].reshape(block_count, ROW_BLOCK, model_dim)

    def block_ffn(block_args):
        hid_blk, exp_idx = block_args
        h_one = jnp.dot(hid_blk, w_one[exp_idx], preferred_element_type=jnp.float32)
        h_three = jnp.dot(hid_blk, w_three[exp_idx], preferred_element_type=jnp.float32)
        act_rows = (jax.nn.silu(h_one) * h_three).astype(jnp.bfloat16)
        return jnp.dot(act_rows, w_two[exp_idx], preferred_element_type=jnp.float32).astype(jnp.bfloat16)

    out_blocks = lax.map(block_ffn, (hidden_blocks, block_exp))
    out_rows = out_blocks.reshape(row_total, model_dim)
    sorted_out = out_rows[dest_row]
    assign_out = jnp.zeros((assign_count, model_dim), jnp.bfloat16).at[sort_order].set(sorted_out)
    both_out = assign_out.reshape(tok_count, 2, model_dim).astype(jnp.float32)
    out_sum = jnp.sum(gate_vals[:, :, None] * both_out, axis=1)
    return out_sum.astype(jnp.bfloat16)
```

```python
import functools

import jax
import jax.numpy as jnp
from jax import lax
from jax.experimental import pallas as pl
from jax.experimental.pallas import tpu as pltpu
from jax.sharding import PartitionSpec as P

MESH = pl.DeviceIdType.MESH
PLANES = 4
SIDE = 8
BUCKET = 64
TILE = 512


def xor_bits(a, b, bits):
    total = 0
    for bit in range(bits):
        step = 1 << bit
        total = total + ((a // step + b // step) % 2) * step
    return total


def moe_kernel(cap, x, pos_row, pos_col, gates, meta, w1, w3, w2, out, ysend, zbuf, metain, bsend, xin, ein, rsend, rin, acc, outacc, wb1, wb3, wb2, wsem, ysem, zsem, msem, mrsem, bsem, xsem, esem, eisem, rsem, rinsem):
    tok, model = x.shape
    rows = SIDE * BUCKET
    n_tiles = w1.shape[2] // TILE
    n_steps = PLANES * n_tiles
    me = lax.axis_index("ep")
    plane, seat = me // SIDE, me % SIDE

    def column_peer(i):
        return xor_bits(plane, i, 2) * SIDE + seat

    def plane_peer(j):
        return plane * SIDE + xor_bits(seat, j, 3)

    def weight_copies(step):
        slot, cols = step % 2, pl.ds(pl.multiple_of((step % n_tiles) * TILE, TILE), TILE)
        return (
            pltpu.make_async_copy(w1.at[0, :, cols], wb1.at[slot], wsem.at[slot, 0]),
            pltpu.make_async_copy(w3.at[0, :, cols], wb3.at[slot], wsem.at[slot, 1]),
            pltpu.make_async_copy(w2.at[0, cols, :], wb2.at[slot], wsem.at[slot, 2]),
        )

    def remote(src, dst, send, recv, peer):
        return pltpu.make_async_remote_copy(src_ref=src, dst_ref=dst, send_sem=send, recv_sem=recv, device_id=(peer,), device_id_type=MESH)

    def y_copy(i):
        return remote(ysend.at[i - 1], zbuf.at[i], ysem.at[i], zsem.at[i], column_peer(i))

    def meta_copy(i):
        return remote(meta.at[i], metain.at[i], msem.at[i], mrsem.at[i], column_peer(i))

    def bucket(j):
        return pl.ds(j * BUCKET, BUCKET)

    def b_copy(i, j):
        return remote(bsend.at[i, bucket(j)], xin.at[i, bucket(j)], bsem.at[i, j], xsem.at[i, j], plane_peer(j))

    def e_copy(i, j):
        return remote(bsend.at[i, bucket(j)], ein.at[i, bucket(j)], esem.at[i, j], eisem.at[i, j], plane_peer(j))

    def r_copy(i):
        return remote(rsend.at[i], rin.at[i], rsem.at[i], rinsem.at[i], column_peer(i))

    for copy in weight_copies(0):
        copy.start()

    barrier = pltpu.get_barrier_semaphore()
    for i in range(1, PLANES):
        pl.semaphore_signal(barrier, inc=1, device_id=(column_peer(i),), device_id_type=MESH)
    for j in range(1, SIDE):
        pl.semaphore_signal(barrier, inc=1, device_id=(plane_peer(j),), device_id_type=MESH)
    pl.semaphore_wait(barrier, PLANES - 1 + SIDE - 1)

    for i in range(1, PLANES):
        meta_copy(i).start()
    metain[0] = meta[0]

    def compact(i):
        want = lax.broadcasted_iota(jnp.int32, (cap, tok), 0)
        hit = (want == pos_row[2 * i : 2 * i + 1, :]) | (want == pos_row[2 * i + 1 : 2 * i + 2, :])
        return jnp.dot(hit.astype(jnp.float32).astype(jnp.bfloat16), x[...], preferred_element_type=jnp.float32).astype(jnp.bfloat16)

    ysend[0] = compact(1)
    ysend[1] = compact(2)
    y_copy(1).start()
    ysend[2] = compact(3)
    y_copy(2).start()
    zbuf[0] = compact(0)
    y_copy(3).start()

    def spread(i):
        diff = lax.broadcasted_iota(jnp.int32, (BUCKET, cap), 1) - lax.broadcasted_iota(jnp.int32, (BUCKET, cap), 0)
        hits = [(diff == metain[i, j : j + 1, :cap]).astype(jnp.float32).astype(jnp.bfloat16) for j in range(SIDE)]
        spread_rows = jnp.dot(jnp.concatenate(hits, axis=0), zbuf[i], preferred_element_type=jnp.float32).astype(jnp.bfloat16)
        bsend[i] = spread_rows
        for j in range(1, SIDE):
            b_copy(i, j).start()

    def collect(i):
        ein[i, 0:BUCKET] = bsend[i, 0:BUCKET]
        for j in range(1, SIDE):
            e_copy(i, j).wait_recv()
        hit = lax.broadcasted_iota(jnp.int32, (cap, rows), 0) == metain[i, SIDE : SIDE + 1, :]
        return jnp.dot(hit.astype(jnp.float32).astype(jnp.bfloat16), ein[i], preferred_element_type=jnp.float32).astype(jnp.bfloat16)

    spread(0)

    def tile_body(i, f, carry):
        step = i * n_tiles + f
        slot = step % 2

        @pl.when(step + 1 < n_steps)
        def _():
            for copy in weight_copies(step + 1):
                copy.start()

        for copy in weight_copies(step):
            copy.wait()
        up = jnp.dot(xin[i], wb1[slot], preferred_element_type=jnp.float32)
        gate = jnp.dot(xin[i], wb3[slot], preferred_element_type=jnp.float32)
        act = (jax.nn.silu(up) * gate).astype(jnp.bfloat16)
        acc[...] += jnp.dot(act, wb2[slot], preferred_element_type=jnp.float32)

        @pl.when((f == 3) & (i + 1 < PLANES))
        def _():
            y_copy(i + 1).wait_recv()
            meta_copy(i + 1).wait_recv()
            spread(i + 1)

        @pl.when((f == 7) & (i == 1))
        def _():
            rin[0] = collect(0)

        @pl.when((f == 7) & (i > 1))
        def _():
            rsend[i - 1] = collect(i - 1)
            r_copy(i - 1).start()

        return carry

    def block_body(i, carry):
        xin[i, 0:BUCKET] = bsend[i, 0:BUCKET]
        for j in range(1, SIDE):
            b_copy(i, j).wait_recv()
        acc[...] = jnp.zeros_like(acc)
        lax.fori_loop(0, n_tiles, functools.partial(tile_body, i), 0)
        for j in range(1, SIDE):
            b_copy(i, j).wait_send()
        bsend[i] = acc[...].astype(jnp.bfloat16)
        for j in range(1, SIDE):
            e_copy(i, j).start()
        return carry

    lax.fori_loop(0, PLANES, block_body, 0)
    rsend[PLANES - 1] = collect(PLANES - 1)
    r_copy(PLANES - 1).start()

    for i in range(PLANES):
        if i > 0:
            r_copy(i).wait_recv()
        seen = lax.broadcasted_iota(jnp.int32, (tok, cap), 1)
        first = (seen == pos_col[:, 2 * i : 2 * i + 1]).astype(jnp.float32).astype(jnp.bfloat16)
        second = (seen == pos_col[:, 2 * i + 1 : 2 * i + 2]).astype(jnp.float32).astype(jnp.bfloat16)
        mixed = gates[:, 0:1] * jnp.dot(first, rin[i], preferred_element_type=jnp.float32)
        mixed += gates[:, 1:2] * jnp.dot(second, rin[i], preferred_element_type=jnp.float32)
        if i == 0:
            outacc[...] = mixed
        elif i < PLANES - 1:
            outacc[...] += mixed
        else:
            out[...] = (outacc[...] + mixed).astype(jnp.bfloat16)

    for i in range(1, PLANES):
        y_copy(i).wait_send()
        meta_copy(i).wait_send()
        r_copy(i).wait_send()
    for i in range(PLANES):
        for j in range(1, SIDE):
            e_copy(i, j).wait_send()


def fused_moe(cap, x, pos_row, pos_col, gates, meta, w1, w3, w2):
    tok, model = x.shape
    rows = SIDE * BUCKET
    bf = jnp.bfloat16
    vmem = pl.BlockSpec(memory_space=pltpu.VMEM)
    hbm = pl.BlockSpec(memory_space=pl.ANY)
    dma = pltpu.SemaphoreType.DMA
    width = w1.shape[2]
    return pl.pallas_call(
        functools.partial(moe_kernel, cap),
        out_shape=jax.ShapeDtypeStruct((tok, model), bf),
        in_specs=[vmem] * 5 + [hbm] * 3,
        out_specs=vmem,
        scratch_shapes=[
            pltpu.VMEM((PLANES - 1, cap, model), bf),
            pltpu.VMEM((PLANES, cap, model), bf),
            pltpu.VMEM((PLANES, 2 * SIDE, rows), jnp.int32),
            pltpu.VMEM((PLANES, rows, model), bf),
            pltpu.VMEM((PLANES, rows, model), bf),
            pltpu.VMEM((PLANES, rows, model), bf),
            pltpu.VMEM((PLANES, cap, model), bf),
            pltpu.VMEM((PLANES, cap, model), bf),
            pltpu.VMEM((rows, model), jnp.float32),
            pltpu.VMEM((tok, model), jnp.float32),
            pltpu.VMEM((2, model, TILE), bf),
            pltpu.VMEM((2, model, TILE), bf),
            pltpu.VMEM((2, TILE, model), bf),
            dma((2, 3)),
            dma((PLANES,)),
            dma((PLANES,)),
            dma((PLANES,)),
            dma((PLANES,)),
            dma((PLANES, SIDE)),
            dma((PLANES, SIDE)),
            dma((PLANES, SIDE)),
            dma((PLANES, SIDE)),
            dma((PLANES,)),
            dma((PLANES,)),
        ],
        compiler_params=pltpu.CompilerParams(collective_id=0, has_side_effects=True, vmem_limit_bytes=67_000_000),
        cost_estimate=pl.CostEstimate(flops=6 * PLANES * rows * model * width, bytes_accessed=3 * PLANES * model * width * 2, transcendentals=0),
    )(x, pos_row, pos_col, gates, meta, w1, w3, w2)


def route(hidden, w_router, ids, me):
    experts = w_router.shape[1]
    tok = ids.shape[0]
    plane, seat = me // SIDE, me % SIDE
    logits = jnp.dot(hidden.astype(jnp.float32), w_router, preferred_element_type=jnp.float32)
    probs = jax.nn.softmax(logits, axis=-1)
    chosen = ids[:, :, None] == jnp.arange(experts)[None, None, :]
    picked = jnp.sum(jnp.where(chosen, probs[:, None, :], 0.0), axis=2)
    gates = picked / jnp.sum(picked, axis=1, keepdims=True)
    named = jnp.any(chosen, axis=1)
    before = (jnp.arange(tok)[:, None] > jnp.arange(tok)[None, :]).astype(jnp.bfloat16)
    rank = (jnp.dot(before, named.astype(jnp.bfloat16), preferred_element_type=jnp.float32) + 0.5).astype(jnp.int32)
    counts = jnp.sum(named.astype(jnp.int32), axis=0)
    lane = jnp.arange(experts)
    start = jnp.sum(jnp.where(lane[None, :] < lane[:, None], counts[None, :], 0), axis=1)
    pos = jnp.sum(jnp.where(chosen, (rank + start[None, :])[:, None, :], 0), axis=2)
    planes = plane ^ jnp.arange(PLANES)
    plane_start = jnp.sum(jnp.where(lane[None, :] == planes[:, None] * SIDE, start[None, :], 0), axis=1)
    mine = (ids // SIDE)[:, None, :] == planes[None, :, None]
    pos_col = jnp.where(mine, pos[:, None, :] - plane_start[None, :, None], -1).reshape(tok, 2 * PLANES)
    dest = planes[:, None] * SIDE + (seat ^ jnp.arange(SIDE))[None, :]
    at_dest = dest[:, :, None] == lane[None, None, :]
    dest_start = jnp.sum(jnp.where(at_dest, start[None, None, :], 0), axis=2) - plane_start[:, None]
    dest_count = jnp.sum(jnp.where(at_dest, counts[None, None, :], 0), axis=2)
    slot = jnp.arange(BUCKET)
    home = jnp.where(slot[None, None, :] < dest_count[:, :, None], dest_start[:, :, None] + slot[None, None, :], -1)
    wide = SIDE * BUCKET
    meta = jnp.concatenate(
        [
            jnp.broadcast_to(dest_start[:, :, None], (PLANES, SIDE, wide)),
            jnp.broadcast_to(home.reshape(PLANES, 1, wide), (PLANES, SIDE, wide)),
        ],
        axis=1,
    )
    most = jnp.max(jnp.sum(counts.reshape(PLANES, SIDE), axis=1))
    return gates, pos_col.T, pos_col, meta, most


CAPS = (512,)


def solution(mesh):
    def device_body(hidden_loc, w_router, ids_loc, w_one, w_three, w_two):
        me = lax.axis_index("ep")
        gates, pos_row, pos_col, meta, most = route(hidden_loc, w_router, ids_loc, me)
        if len(CAPS) == 1:
            return fused_moe(CAPS[0], hidden_loc, pos_row, pos_col, gates, meta, w_one, w_three, w_two)
        most = lax.pmax(most, "ep")
        pick = sum((most > cap).astype(jnp.int32) for cap in CAPS[:-1])
        branches = [functools.partial(fused_moe, cap) for cap in CAPS]
        return lax.switch(pick, branches, hidden_loc, pos_row, pos_col, gates, meta, w_one, w_three, w_two)

    return jax.shard_map(device_body, mesh=mesh, in_specs=(P("ep", None), P(None, None), P("ep", None), P("ep", None, None), P("ep", None, None), P("ep", None, None)), out_specs=P("ep", None), check_vma=False)
```

```python
import functools

import jax
import jax.numpy as jnp
from jax import lax
from jax.experimental import pallas as pl
from jax.experimental.pallas import tpu as pltpu
from jax.sharding import PartitionSpec as P

MESH = pl.DeviceIdType.MESH
PLANES = 4
SIDE = 8
BUCKET = 64
TILE = 512


def xor_bits(a, b, bits):
    total = 0
    for bit in range(bits):
        step = 1 << bit
        total = total + ((a // step + b // step) % 2) * step
    return total


def moe_kernel(cap, x, pos_row, pos_col, gates, meta, w1, w3, w2, out, ysend, zbuf, metain, bsend, xin, ein, rsend, rin, acc, outacc, wb1, wb3, wb2, wsem, ysem, zsem, msem, mrsem, bsem, xsem, esem, eisem, rsem, rinsem):
    tok, model = x.shape
    rows = SIDE * BUCKET
    n_tiles = w1.shape[2] // TILE
    n_steps = PLANES * n_tiles
    me = lax.axis_index("ep")
    plane, seat = me // SIDE, me % SIDE

    def column_peer(i):
        return xor_bits(plane, i, 2) * SIDE + seat

    def plane_peer(j):
        return plane * SIDE + xor_bits(seat, j, 3)

    def weight_copies(step):
        slot, cols = step % 2, pl.ds(pl.multiple_of((step % n_tiles) * TILE, TILE), TILE)
        return (
            pltpu.make_async_copy(w1.at[0, :, cols], wb1.at[slot], wsem.at[slot, 0]),
            pltpu.make_async_copy(w3.at[0, :, cols], wb3.at[slot], wsem.at[slot, 1]),
            pltpu.make_async_copy(w2.at[0, cols, :], wb2.at[slot], wsem.at[slot, 2]),
        )

    def remote(src, dst, send, recv, peer):
        return pltpu.make_async_remote_copy(src_ref=src, dst_ref=dst, send_sem=send, recv_sem=recv, device_id=(peer,), device_id_type=MESH)

    def y_copy(i):
        return remote(ysend.at[i], zbuf.at[i - 1], ysem.at[i], zsem.at[i], column_peer(i))

    def meta_copy(i):
        return remote(meta.at[i], metain.at[i], msem.at[i], mrsem.at[i], column_peer(i))

    def bucket(j):
        return pl.ds(j * BUCKET, BUCKET)

    def b_copy(i, j):
        return remote(bsend.at[i, bucket(j)], xin.at[i, bucket(j)], bsem.at[i, j], xsem.at[i, j], plane_peer(j))

    def e_copy(i, j):
        return remote(bsend.at[i, bucket(j)], ein.at[i, bucket(j)], esem.at[i, j], eisem.at[i, j], plane_peer(j))

    def r_copy(i):
        return remote(rsend.at[i], rin.at[i], rsem.at[i], rinsem.at[i], column_peer(i))

    for copy in weight_copies(0):
        copy.start()

    barrier = pltpu.get_barrier_semaphore()
    for i in range(1, PLANES):
        pl.semaphore_signal(barrier, inc=1, device_id=(column_peer(i),), device_id_type=MESH)
    for j in range(1, SIDE):
        pl.semaphore_signal(barrier, inc=1, device_id=(plane_peer(j),), device_id_type=MESH)
    pl.semaphore_wait(barrier, PLANES - 1 + SIDE - 1)

    for i in range(1, PLANES):
        meta_copy(i).start()
    metain[0] = meta[0]

    def compact(i):
        want = lax.broadcasted_iota(jnp.int32, (cap, tok), 0)
        where = pos_row[i]
        hit = (want == where[0:1, :]) | (want == where[1:2, :])
        return jnp.dot(hit.astype(jnp.float32).astype(jnp.bfloat16), x[...], preferred_element_type=jnp.float32).astype(jnp.bfloat16)

    def compact_body(n, carry):
        i = (n + 1) % PLANES
        ysend[i] = compact(i)

        @pl.when(n > 0)
        def _():
            y_copy(n).start()

        return carry

    lax.fori_loop(0, PLANES, compact_body, 0)

    def spread(i, arrived):
        diff = lax.broadcasted_iota(jnp.int32, (BUCKET, cap), 1) - lax.broadcasted_iota(jnp.int32, (BUCKET, cap), 0)
        hits = [(diff == metain[i, j : j + 1, :cap]).astype(jnp.float32).astype(jnp.bfloat16) for j in range(SIDE)]
        spread_rows = jnp.dot(jnp.concatenate(hits, axis=0), arrived[...], preferred_element_type=jnp.float32).astype(jnp.bfloat16)
        bsend[i] = spread_rows
        for j in range(1, SIDE):
            b_copy(i, j).start()

    def collect(i):
        ein[i, 0:BUCKET] = bsend[i, 0:BUCKET]
        for j in range(1, SIDE):
            e_copy(i, j).wait_recv()
        hit = lax.broadcasted_iota(jnp.int32, (cap, rows), 0) == metain[i, SIDE : SIDE + 1, :]
        return jnp.dot(hit.astype(jnp.float32).astype(jnp.bfloat16), ein[i], preferred_element_type=jnp.float32).astype(jnp.bfloat16)

    spread(0, ysend.at[0])

    def tile_body(i, f, carry):
        step = i * n_tiles + f
        slot = step % 2

        @pl.when(step + 1 < n_steps)
        def _():
            for copy in weight_copies(step + 1):
                copy.start()

        for copy in weight_copies(step):
            copy.wait()
        up = jnp.dot(xin[i], wb1[slot], preferred_element_type=jnp.float32)
        gate = jnp.dot(xin[i], wb3[slot], preferred_element_type=jnp.float32)
        act = (jax.nn.silu(up) * gate).astype(jnp.bfloat16)
        acc[...] += jnp.dot(act, wb2[slot], preferred_element_type=jnp.float32)

        @pl.when((f == 3) & (i + 1 < PLANES))
        def _():
            y_copy(i + 1).wait_recv()
            meta_copy(i + 1).wait_recv()
            spread(i + 1, zbuf.at[i])

        @pl.when((f == 7) & (i > 0))
        def _():
            rsend[i - 1] = collect(i - 1)

        @pl.when((f == 7) & (i > 1))
        def _():
            r_copy(i - 1).start()

        @pl.when((f == 8) & (i == 1))
        def _():
            rin[0] = rsend[0]

        return carry

    def block_body(i, carry):
        xin[i, 0:BUCKET] = bsend[i, 0:BUCKET]
        for j in range(1, SIDE):
            b_copy(i, j).wait_recv()
        acc[...] = jnp.zeros_like(acc)
        lax.fori_loop(0, n_tiles, functools.partial(tile_body, i), 0)
        for j in range(1, SIDE):
            b_copy(i, j).wait_send()
        bsend[i] = acc[...].astype(jnp.bfloat16)
        for j in range(1, SIDE):
            e_copy(i, j).start()
        return carry

    lax.fori_loop(0, PLANES, block_body, 0)
    rsend[PLANES - 1] = collect(PLANES - 1)
    r_copy(PLANES - 1).start()

    def mix(i, results):
        seen = lax.broadcasted_iota(jnp.int32, (tok, cap), 1)
        where = pos_col[i]
        first = (seen == where[:, 0:1]).astype(jnp.float32).astype(jnp.bfloat16)
        second = (seen == where[:, 1:2]).astype(jnp.float32).astype(jnp.bfloat16)
        mixed = gates[:, 0:1] * jnp.dot(first, results, preferred_element_type=jnp.float32)
        return mixed + gates[:, 1:2] * jnp.dot(second, results, preferred_element_type=jnp.float32)

    outacc[...] = jnp.zeros_like(outacc)

    def mix_body(i, carry):
        @pl.when(i > 0)
        def _():
            r_copy(i).wait_recv()

        outacc[...] += mix(i, rin[i])
        return carry

    lax.fori_loop(0, PLANES, mix_body, 0)
    out[...] = outacc[...].astype(jnp.bfloat16)

    for i in range(1, PLANES):
        y_copy(i).wait_send()
        meta_copy(i).wait_send()
        r_copy(i).wait_send()
    for i in range(PLANES):
        for j in range(1, SIDE):
            e_copy(i, j).wait_send()


def fused_moe(cap, x, pos_row, pos_col, gates, meta, w1, w3, w2):
    tok, model = x.shape
    rows = SIDE * BUCKET
    bf = jnp.bfloat16
    vmem = pl.BlockSpec(memory_space=pltpu.VMEM)
    hbm = pl.BlockSpec(memory_space=pl.ANY)
    dma = pltpu.SemaphoreType.DMA
    width = w1.shape[2]
    return pl.pallas_call(
        functools.partial(moe_kernel, cap),
        out_shape=jax.ShapeDtypeStruct((tok, model), bf),
        in_specs=[vmem] * 5 + [hbm] * 3,
        out_specs=vmem,
        scratch_shapes=[
            pltpu.VMEM((PLANES, cap, model), bf),
            pltpu.VMEM((PLANES - 1, cap, model), bf),
            pltpu.VMEM((PLANES, 2 * SIDE, rows), jnp.int32),
            pltpu.VMEM((PLANES, rows, model), bf),
            pltpu.VMEM((PLANES, rows, model), bf),
            pltpu.VMEM((PLANES, rows, model), bf),
            pltpu.VMEM((PLANES, cap, model), bf),
            pltpu.VMEM((PLANES, cap, model), bf),
            pltpu.VMEM((rows, model), jnp.float32),
            pltpu.VMEM((tok, model), jnp.float32),
            pltpu.VMEM((2, model, TILE), bf),
            pltpu.VMEM((2, model, TILE), bf),
            pltpu.VMEM((2, TILE, model), bf),
            dma((2, 3)),
            dma((PLANES,)),
            dma((PLANES,)),
            dma((PLANES,)),
            dma((PLANES,)),
            dma((PLANES, SIDE)),
            dma((PLANES, SIDE)),
            dma((PLANES, SIDE)),
            dma((PLANES, SIDE)),
            dma((PLANES,)),
            dma((PLANES,)),
        ],
        compiler_params=pltpu.CompilerParams(collective_id=0, has_side_effects=True, vmem_limit_bytes=67_000_000),
        cost_estimate=pl.CostEstimate(flops=6 * PLANES * rows * model * width, bytes_accessed=3 * PLANES * model * width * 2, transcendentals=0),
    )(x, pos_row, pos_col, gates, meta, w1, w3, w2)


def route(hidden, w_router, ids, me):
    experts = w_router.shape[1]
    tok = ids.shape[0]
    plane, seat = me // SIDE, me % SIDE
    logits = jnp.dot(hidden.astype(jnp.float32), w_router, preferred_element_type=jnp.float32)
    probs = jax.nn.softmax(logits, axis=-1)
    chosen = ids[:, :, None] == jnp.arange(experts)[None, None, :]
    picked = jnp.sum(jnp.where(chosen, probs[:, None, :], 0.0), axis=2)
    gates = picked / jnp.sum(picked, axis=1, keepdims=True)
    named = jnp.any(chosen, axis=1)
    before = (jnp.arange(tok)[:, None] > jnp.arange(tok)[None, :]).astype(jnp.bfloat16)
    rank = (jnp.dot(before, named.astype(jnp.bfloat16), preferred_element_type=jnp.float32) + 0.5).astype(jnp.int32)
    counts = jnp.sum(named.astype(jnp.int32), axis=0)
    lane = jnp.arange(experts)
    start = jnp.sum(jnp.where(lane[None, :] < lane[:, None], counts[None, :], 0), axis=1)
    pos = jnp.sum(jnp.where(chosen, (rank + start[None, :])[:, None, :], 0), axis=2)
    planes = plane ^ jnp.arange(PLANES)
    plane_start = jnp.sum(jnp.where(lane[None, :] == planes[:, None] * SIDE, start[None, :], 0), axis=1)
    mine = (ids // SIDE).T[None, :, :] == planes[:, None, None]
    pos_row = jnp.where(mine, pos.T[None, :, :] - plane_start[:, None, None], -1)
    dest = planes[:, None] * SIDE + (seat ^ jnp.arange(SIDE))[None, :]
    at_dest = dest[:, :, None] == lane[None, None, :]
    dest_start = jnp.sum(jnp.where(at_dest, start[None, None, :], 0), axis=2) - plane_start[:, None]
    dest_count = jnp.sum(jnp.where(at_dest, counts[None, None, :], 0), axis=2)
    slot = jnp.arange(BUCKET)
    home = jnp.where(slot[None, None, :] < dest_count[:, :, None], dest_start[:, :, None] + slot[None, None, :], -1)
    wide = SIDE * BUCKET
    meta = jnp.concatenate(
        [
            jnp.broadcast_to(dest_start[:, :, None], (PLANES, SIDE, wide)),
            jnp.broadcast_to(home.reshape(PLANES, 1, wide), (PLANES, SIDE, wide)),
        ],
        axis=1,
    )
    most = jnp.max(jnp.sum(counts.reshape(PLANES, SIDE), axis=1))
    return gates, pos_row, pos_row.transpose(0, 2, 1), meta, most


CAPS = (304, 352, 512)


def solution(mesh):
    def device_body(hidden_loc, w_router, ids_loc, w_one, w_three, w_two):
        me = lax.axis_index("ep")
        gates, pos_row, pos_col, meta, most = route(hidden_loc, w_router, ids_loc, me)
        if len(CAPS) == 1:
            return fused_moe(CAPS[0], hidden_loc, pos_row, pos_col, gates, meta, w_one, w_three, w_two)
        most = lax.pmax(most, "ep")
        pick = sum((most > cap).astype(jnp.int32) for cap in CAPS[:-1])
        branches = [functools.partial(fused_moe, cap) for cap in CAPS]
        return lax.switch(pick, branches, hidden_loc, pos_row, pos_col, gates, meta, w_one, w_three, w_two)

    return jax.shard_map(device_body, mesh=mesh, in_specs=(P("ep", None), P(None, None), P("ep", None), P("ep", None, None), P("ep", None, None), P("ep", None, None)), out_specs=P("ep", None), check_vma=False)
```

```python
import functools

import jax
import jax.numpy as jnp
from jax import lax
from jax.experimental import pallas as pl
from jax.experimental.pallas import tpu as pltpu
from jax.sharding import PartitionSpec as P

MESH = pl.DeviceIdType.MESH
PLANES = 4
SIDE = 8
BUCKET = 64
TILE = 512
SEND_ORDER = (6, 7, 4, 2, 5, 3, 1)


def xor_bits(a, b, bits):
    total = 0
    for bit in range(bits):
        step = 1 << bit
        total = total + ((a // step + b // step) % 2) * step
    return total


def moe_kernel(cap, x, pos_row, pos_col, gates, meta, w1, w3, w2, out, ysend, zbuf, metain, bsend, xin, ein, rsend, rin, acc, outacc, wb1, wb3, wb2, wsem, ysem, zsem, msem, mrsem, bsem, xsem, esem, eisem, rsem, rinsem):
    tok, model = x.shape
    rows = SIDE * BUCKET
    n_tiles = w1.shape[2] // TILE
    n_steps = PLANES * n_tiles
    me = lax.axis_index("ep")
    plane, seat = me // SIDE, me % SIDE

    def column_peer(i):
        return xor_bits(plane, i, 2) * SIDE + seat

    def plane_peer(j):
        return plane * SIDE + xor_bits(seat, j, 3)

    def weight_copies(step):
        slot, cols = step % 2, pl.ds(pl.multiple_of((step % n_tiles) * TILE, TILE), TILE)
        return (
            pltpu.make_async_copy(w1.at[0, :, cols], wb1.at[slot], wsem.at[slot, 0]),
            pltpu.make_async_copy(w3.at[0, :, cols], wb3.at[slot], wsem.at[slot, 1]),
            pltpu.make_async_copy(w2.at[0, cols, :], wb2.at[slot], wsem.at[slot, 2]),
        )

    def remote(src, dst, send, recv, peer):
        return pltpu.make_async_remote_copy(src_ref=src, dst_ref=dst, send_sem=send, recv_sem=recv, device_id=(peer,), device_id_type=MESH)

    def y_copy(i):
        return remote(ysend.at[i], zbuf.at[i - 1], ysem.at[i], zsem.at[i], column_peer(i))

    def meta_copy(i):
        return remote(meta.at[i], metain.at[i], msem.at[i], mrsem.at[i], column_peer(i))

    def bucket(j):
        return pl.ds(j * BUCKET, BUCKET)

    def b_copy(i, j):
        return remote(bsend.at[i, bucket(j)], xin.at[i, bucket(j)], bsem.at[i, j], xsem.at[i, j], plane_peer(j))

    def e_copy(i, j):
        return remote(bsend.at[i, bucket(j)], ein.at[i, bucket(j)], esem.at[i, j], eisem.at[i, j], plane_peer(j))

    def r_copy(i):
        return remote(rsend.at[i], rin.at[i], rsem.at[i], rinsem.at[i], column_peer(i))

    for copy in weight_copies(0):
        copy.start()

    barrier = pltpu.get_barrier_semaphore()
    for i in range(1, PLANES):
        pl.semaphore_signal(barrier, inc=1, device_id=(column_peer(i),), device_id_type=MESH)
    for j in range(1, SIDE):
        pl.semaphore_signal(barrier, inc=1, device_id=(plane_peer(j),), device_id_type=MESH)
    pl.semaphore_wait(barrier, PLANES - 1 + SIDE - 1)

    for i in range(1, PLANES):
        meta_copy(i).start()
    metain[0] = meta[0]

    def compact(i):
        want = lax.broadcasted_iota(jnp.int32, (cap, tok), 0)
        where = pos_row[i]
        hit = (want == where[0:1, :]) | (want == where[1:2, :])
        return jnp.dot(hit.astype(jnp.float32).astype(jnp.bfloat16), x[...], preferred_element_type=jnp.float32).astype(jnp.bfloat16)

    def compact_body(n, carry):
        i = (n + 1) % PLANES
        ysend[i] = compact(i)

        @pl.when(n > 0)
        def _():
            y_copy(n).start()

        return carry

    lax.fori_loop(0, PLANES, compact_body, 0)

    def spread(i, arrived):
        diff = lax.broadcasted_iota(jnp.int32, (BUCKET, cap), 1) - lax.broadcasted_iota(jnp.int32, (BUCKET, cap), 0)
        hits = [(diff == metain[i, j : j + 1, :cap]).astype(jnp.float32).astype(jnp.bfloat16) for j in range(SIDE)]
        spread_rows = jnp.dot(jnp.concatenate(hits, axis=0), arrived[...], preferred_element_type=jnp.float32).astype(jnp.bfloat16)
        bsend[i] = spread_rows
        for j in SEND_ORDER:
            b_copy(i, j).start()

    def collect(i):
        ein[i, 0:BUCKET] = bsend[i, 0:BUCKET]
        for j in range(1, SIDE):
            e_copy(i, j).wait_recv()
        hit = lax.broadcasted_iota(jnp.int32, (cap, rows), 0) == metain[i, SIDE : SIDE + 1, :]
        return jnp.dot(hit.astype(jnp.float32).astype(jnp.bfloat16), ein[i], preferred_element_type=jnp.float32).astype(jnp.bfloat16)

    spread(0, ysend.at[0])

    def tile_body(i, f, carry):
        step = i * n_tiles + f
        slot = step % 2

        @pl.when(step + 1 < n_steps)
        def _():
            for copy in weight_copies(step + 1):
                copy.start()

        for copy in weight_copies(step):
            copy.wait()
        up = jnp.dot(xin[i], wb1[slot], preferred_element_type=jnp.float32)
        gate = jnp.dot(xin[i], wb3[slot], preferred_element_type=jnp.float32)
        act = (jax.nn.silu(up) * gate).astype(jnp.bfloat16)
        acc[...] += jnp.dot(act, wb2[slot], preferred_element_type=jnp.float32)

        @pl.when((f == 3) & (i + 1 < PLANES))
        def _():
            y_copy(i + 1).wait_recv()
            meta_copy(i + 1).wait_recv()
            spread(i + 1, zbuf.at[i])

        @pl.when((f == 7) & (i > 0))
        def _():
            rsend[i - 1] = collect(i - 1)

        @pl.when((f == 7) & (i > 1))
        def _():
            r_copy(i - 1).start()

        @pl.when((f == 8) & (i == 1))
        def _():
            rin[0] = rsend[0]

        return carry

    def block_body(i, carry):
        xin[i, 0:BUCKET] = bsend[i, 0:BUCKET]
        for j in range(1, SIDE):
            b_copy(i, j).wait_recv()
        acc[...] = jnp.zeros_like(acc)
        lax.fori_loop(0, n_tiles, functools.partial(tile_body, i), 0)
        for j in range(1, SIDE):
            b_copy(i, j).wait_send()
        bsend[i] = acc[...].astype(jnp.bfloat16)
        for j in SEND_ORDER:
            e_copy(i, j).start()
        return carry

    lax.fori_loop(0, PLANES, block_body, 0)
    rsend[PLANES - 1] = collect(PLANES - 1)
    r_copy(PLANES - 1).start()

    def mix(i, results):
        seen = lax.broadcasted_iota(jnp.int32, (tok, cap), 1).astype(jnp.float32)
        lane = lax.broadcasted_iota(jnp.int32, (tok, 2 * PLANES), 1)
        where = [jnp.sum(jnp.where(lane == 2 * i + k, pos_col[...], 0.0), axis=1, keepdims=True) for k in range(2)]
        first = (seen == where[0]).astype(jnp.float32).astype(jnp.bfloat16)
        second = (seen == where[1]).astype(jnp.float32).astype(jnp.bfloat16)
        mixed = gates[:, 0:1] * jnp.dot(first, results, preferred_element_type=jnp.float32)
        return mixed + gates[:, 1:2] * jnp.dot(second, results, preferred_element_type=jnp.float32)

    outacc[...] = jnp.zeros_like(outacc)

    def mix_body(i, carry):
        @pl.when(i > 0)
        def _():
            r_copy(i).wait_recv()

        outacc[...] += mix(i, rin[i])
        return carry

    lax.fori_loop(0, PLANES, mix_body, 0)
    out[...] = outacc[...].astype(jnp.bfloat16)

    for i in range(1, PLANES):
        y_copy(i).wait_send()
        meta_copy(i).wait_send()
        r_copy(i).wait_send()
    for i in range(PLANES):
        for j in range(1, SIDE):
            e_copy(i, j).wait_send()


def fused_moe(cap, x, pos_row, pos_col, gates, meta, w1, w3, w2):
    tok, model = x.shape
    rows = SIDE * BUCKET
    bf = jnp.bfloat16
    vmem = pl.BlockSpec(memory_space=pltpu.VMEM)
    hbm = pl.BlockSpec(memory_space=pl.ANY)
    dma = pltpu.SemaphoreType.DMA
    width = w1.shape[2]
    return pl.pallas_call(
        functools.partial(moe_kernel, cap),
        out_shape=jax.ShapeDtypeStruct((tok, model), bf),
        in_specs=[vmem] * 5 + [hbm] * 3,
        out_specs=vmem,
        scratch_shapes=[
            pltpu.VMEM((PLANES, cap, model), bf),
            pltpu.VMEM((PLANES - 1, cap, model), bf),
            pltpu.VMEM((PLANES, 2 * SIDE, rows), jnp.int32),
            pltpu.VMEM((PLANES, rows, model), bf),
            pltpu.VMEM((PLANES, rows, model), bf),
            pltpu.VMEM((PLANES, rows, model), bf),
            pltpu.VMEM((PLANES, cap, model), bf),
            pltpu.VMEM((PLANES, cap, model), bf),
            pltpu.VMEM((rows, model), jnp.float32),
            pltpu.VMEM((tok, model), jnp.float32),
            pltpu.VMEM((2, model, TILE), bf),
            pltpu.VMEM((2, model, TILE), bf),
            pltpu.VMEM((2, TILE, model), bf),
            dma((2, 3)),
            dma((PLANES,)),
            dma((PLANES,)),
            dma((PLANES,)),
            dma((PLANES,)),
            dma((PLANES, SIDE)),
            dma((PLANES, SIDE)),
            dma((PLANES, SIDE)),
            dma((PLANES, SIDE)),
            dma((PLANES,)),
            dma((PLANES,)),
        ],
        compiler_params=pltpu.CompilerParams(collective_id=0, has_side_effects=True, vmem_limit_bytes=67_000_000),
        cost_estimate=pl.CostEstimate(flops=6 * PLANES * rows * model * width, bytes_accessed=3 * PLANES * model * width * 2, transcendentals=0),
    )(x, pos_row, pos_col, gates, meta, w1, w3, w2)


def peak_kernel(n, mine, out, heard, ssem, rsem):
    me = lax.axis_index("ep")

    def copy(k):
        return pltpu.make_async_remote_copy(src_ref=mine, dst_ref=heard.at[k], send_sem=ssem.at[k], recv_sem=rsem.at[k], device_id=((me + k) % n,), device_id_type=MESH)

    barrier = pltpu.get_barrier_semaphore()
    for k in range(1, n):
        pl.semaphore_signal(barrier, inc=1, device_id=((me + k) % n,), device_id_type=MESH)
    pl.semaphore_wait(barrier, n - 1)
    for k in range(1, n):
        copy(k).start()
    heard[0] = mine[...]
    for k in range(1, n):
        copy(k).wait_recv()
    out[...] = jnp.max(heard[...], axis=0)
    for k in range(1, n):
        copy(k).wait_send()


def global_peak(n, most):
    vmem = pl.BlockSpec(memory_space=pltpu.VMEM)
    shape = (8, 128)
    peaks = pl.pallas_call(
        functools.partial(peak_kernel, n),
        out_shape=jax.ShapeDtypeStruct(shape, jnp.int32),
        in_specs=[vmem],
        out_specs=vmem,
        scratch_shapes=[pltpu.VMEM((n,) + shape, jnp.int32), pltpu.SemaphoreType.DMA((n,)), pltpu.SemaphoreType.DMA((n,))],
        compiler_params=pltpu.CompilerParams(collective_id=1, has_side_effects=True),
    )(jnp.full(shape, most, jnp.int32))
    return peaks[0, 0]


def route(hidden, w_router, ids, me):
    experts = w_router.shape[1]
    tok = ids.shape[0]
    plane, seat = me // SIDE, me % SIDE
    logits = jnp.dot(hidden.astype(jnp.float32), w_router, preferred_element_type=jnp.float32)
    probs = jax.nn.softmax(logits, axis=-1)
    chosen = ids[:, :, None] == jnp.arange(experts)[None, None, :]
    picked = jnp.sum(jnp.where(chosen, probs[:, None, :], 0.0), axis=2)
    gates = picked / jnp.sum(picked, axis=1, keepdims=True)
    named = jnp.any(chosen, axis=1)
    before = (jnp.arange(tok)[:, None] > jnp.arange(tok)[None, :]).astype(jnp.bfloat16)
    rank = (jnp.dot(before, named.astype(jnp.bfloat16), preferred_element_type=jnp.float32) + 0.5).astype(jnp.int32)
    counts = jnp.sum(named.astype(jnp.int32), axis=0)
    lane = jnp.arange(experts)
    start = jnp.sum(jnp.where(lane[None, :] < lane[:, None], counts[None, :], 0), axis=1)
    pos = jnp.sum(jnp.where(chosen, (rank + start[None, :])[:, None, :], 0), axis=2)
    planes = plane ^ jnp.arange(PLANES)
    plane_start = jnp.sum(jnp.where(lane[None, :] == planes[:, None] * SIDE, start[None, :], 0), axis=1)
    mine = (ids // SIDE)[:, None, :] == planes[None, :, None]
    pos_col = jnp.where(mine, pos[:, None, :] - plane_start[None, :, None], -1).reshape(tok, 2 * PLANES)
    dest = planes[:, None] * SIDE + (seat ^ jnp.arange(SIDE))[None, :]
    at_dest = dest[:, :, None] == lane[None, None, :]
    dest_start = jnp.sum(jnp.where(at_dest, start[None, None, :], 0), axis=2) - plane_start[:, None]
    dest_count = jnp.sum(jnp.where(at_dest, counts[None, None, :], 0), axis=2)
    slot = jnp.arange(BUCKET)
    home = jnp.where(slot[None, None, :] < dest_count[:, :, None], dest_start[:, :, None] + slot[None, None, :], -1)
    wide = SIDE * BUCKET
    meta = jnp.concatenate(
        [
            jnp.broadcast_to(dest_start[:, :, None], (PLANES, SIDE, wide)),
            jnp.broadcast_to(home.reshape(PLANES, 1, wide), (PLANES, SIDE, wide)),
        ],
        axis=1,
    )
    most = jnp.max(jnp.sum(counts.reshape(PLANES, SIDE), axis=1))
    return gates, pos_col.T.reshape(PLANES, 2, tok), pos_col.astype(jnp.float32), meta, most


CAPS = (304, 352, 512)


def solution(mesh):
    def device_body(hidden_loc, w_router, ids_loc, w_one, w_three, w_two):
        me = lax.axis_index("ep")
        gates, pos_row, pos_col, meta, most = route(hidden_loc, w_router, ids_loc, me)
        if len(CAPS) == 1:
            return fused_moe(CAPS[0], hidden_loc, pos_row, pos_col, gates, meta, w_one, w_three, w_two)
        most = global_peak(mesh.shape["ep"], most)
        pick = sum((most > cap).astype(jnp.int32) for cap in CAPS[:-1])
        branches = [functools.partial(fused_moe, cap) for cap in CAPS]
        return lax.switch(pick, branches, hidden_loc, pos_row, pos_col, gates, meta, w_one, w_three, w_two)

    return jax.shard_map(device_body, mesh=mesh, in_specs=(P("ep", None), P(None, None), P("ep", None), P("ep", None, None), P("ep", None, None), P("ep", None, None)), out_specs=P("ep", None), check_vma=False)
```

```python
import functools

import jax
import jax.numpy as jnp
from jax import lax
from jax.experimental import pallas as pl
from jax.experimental.pallas import tpu as pltpu
from jax.sharding import PartitionSpec as P

MESH = pl.DeviceIdType.MESH
PLANES = 4
SIDE = 8
BUCKET = 64
TILE = 512
SEND_ORDER = (6, 7, 4, 2, 5, 3, 1)


def xor_bits(a, b, bits):
    total = 0
    for bit in range(bits):
        step = 1 << bit
        total = total + ((a // step + b // step) % 2) * step
    return total


def moe_kernel(cap, x, pos_row, pos_col, gates, meta, w1, w3, w2, out, ysend, zbuf, metain, bsend, xin, ein, rsend, rin, acc, outacc, wb1, wb3, wb2, wsem, ysem, zsem, msem, mrsem, bsem, xsem, esem, eisem, rsem, rinsem):
    tok, model = x.shape
    rows = SIDE * BUCKET
    n_tiles = w1.shape[2] // TILE
    n_steps = PLANES * n_tiles
    me = lax.axis_index("ep")
    plane, seat = me // SIDE, me % SIDE

    def column_peer(i):
        return xor_bits(plane, i, 2) * SIDE + seat

    def plane_peer(j):
        return plane * SIDE + xor_bits(seat, j, 3)

    def weight_copies(step):
        slot, cols = step % 2, pl.ds(pl.multiple_of((step % n_tiles) * TILE, TILE), TILE)
        return (
            pltpu.make_async_copy(w1.at[0, :, cols], wb1.at[slot], wsem.at[slot, 0]),
            pltpu.make_async_copy(w3.at[0, :, cols], wb3.at[slot], wsem.at[slot, 1]),
            pltpu.make_async_copy(w2.at[0, cols, :], wb2.at[slot], wsem.at[slot, 2]),
        )

    def remote(src, dst, send, recv, peer):
        return pltpu.make_async_remote_copy(src_ref=src, dst_ref=dst, send_sem=send, recv_sem=recv, device_id=(peer,), device_id_type=MESH)

    def y_copy(i):
        return remote(ysend.at[i], zbuf.at[i - 1], ysem.at[i], zsem.at[i], column_peer(i))

    def meta_copy(i):
        return remote(meta.at[i], metain.at[i], msem.at[i], mrsem.at[i], column_peer(i))

    def bucket(j):
        return pl.ds(j * BUCKET, BUCKET)

    def b_copy(i, j):
        return remote(bsend.at[i, bucket(j)], xin.at[i, bucket(j)], bsem.at[i, j], xsem.at[i, j], plane_peer(j))

    def e_copy(i, j):
        return remote(bsend.at[i, bucket(j)], ein.at[i, bucket(j)], esem.at[i, j], eisem.at[i, j], plane_peer(j))

    def r_copy(i):
        return remote(rsend.at[i], rin.at[i], rsem.at[i], rinsem.at[i], column_peer(i))

    for copy in weight_copies(0):
        copy.start()

    barrier = pltpu.get_barrier_semaphore()
    for i in range(1, PLANES):
        pl.semaphore_signal(barrier, inc=1, device_id=(column_peer(i),), device_id_type=MESH)
    for j in range(1, SIDE):
        pl.semaphore_signal(barrier, inc=1, device_id=(plane_peer(j),), device_id_type=MESH)
    pl.semaphore_wait(barrier, PLANES - 1 + SIDE - 1)

    for i in range(1, PLANES):
        meta_copy(i).start()
    metain[0] = meta[0]

    def compact(i):
        want = lax.broadcasted_iota(jnp.int32, (cap, tok), 0)
        where = pos_row[i]
        hit = (want == where[0:1, :]) | (want == where[1:2, :])
        return jnp.dot(hit.astype(jnp.float32).astype(jnp.bfloat16), x[...], preferred_element_type=jnp.float32).astype(jnp.bfloat16)

    def compact_body(n, carry):
        i = (n + 1) % PLANES
        ysend[i] = compact(i)

        @pl.when(n > 0)
        def _():
            y_copy(n).start()

        return carry

    lax.fori_loop(0, PLANES, compact_body, 0)

    def spread(i, arrived):
        diff = lax.broadcasted_iota(jnp.int32, (BUCKET, cap), 1) - lax.broadcasted_iota(jnp.int32, (BUCKET, cap), 0)
        hits = [(diff == metain[i, j : j + 1, :cap]).astype(jnp.float32).astype(jnp.bfloat16) for j in range(SIDE)]
        spread_rows = jnp.dot(jnp.concatenate(hits, axis=0), arrived[...], preferred_element_type=jnp.float32).astype(jnp.bfloat16)
        bsend[i] = spread_rows
        for j in SEND_ORDER:
            b_copy(i, j).start()

    def collect(i):
        ein[i, 0:BUCKET] = bsend[i, 0:BUCKET]
        for j in range(1, SIDE):
            e_copy(i, j).wait_recv()
        hit = lax.broadcasted_iota(jnp.int32, (cap, rows), 0) == metain[i, SIDE : SIDE + 1, :]
        return jnp.dot(hit.astype(jnp.float32).astype(jnp.bfloat16), ein[i], preferred_element_type=jnp.float32).astype(jnp.bfloat16)

    spread(0, ysend.at[0])

    def tile_body(i, f, carry):
        step = i * n_tiles + f
        slot = step % 2

        @pl.when(step + 1 < n_steps)
        def _():
            for copy in weight_copies(step + 1):
                copy.start()

        for copy in weight_copies(step):
            copy.wait()
        up = jnp.dot(xin[i], wb1[slot], preferred_element_type=jnp.float32)
        gate = jnp.dot(xin[i], wb3[slot], preferred_element_type=jnp.float32)
        act = (jax.nn.silu(up) * gate).astype(jnp.bfloat16)
        acc[...] += jnp.dot(act, wb2[slot], preferred_element_type=jnp.float32)

        @pl.when((f == 3) & (i + 1 < PLANES))
        def _():
            y_copy(i + 1).wait_recv()
            meta_copy(i + 1).wait_recv()
            spread(i + 1, zbuf.at[i])

        @pl.when((f == 7) & (i > 0))
        def _():
            rsend[i - 1] = collect(i - 1)

        @pl.when((f == 7) & (i > 1))
        def _():
            r_copy(i - 1).start()

        @pl.when((f == 8) & (i == 1))
        def _():
            rin[0] = rsend[0]

        return carry

    def block_body(i, carry):
        xin[i, 0:BUCKET] = bsend[i, 0:BUCKET]
        for j in range(1, SIDE):
            b_copy(i, j).wait_recv()
        acc[...] = jnp.zeros_like(acc)
        lax.fori_loop(0, n_tiles, functools.partial(tile_body, i), 0)
        for j in range(1, SIDE):
            b_copy(i, j).wait_send()
        bsend[i] = acc[...].astype(jnp.bfloat16)
        for j in SEND_ORDER:
            e_copy(i, j).start()
        return carry

    lax.fori_loop(0, PLANES, block_body, 0)
    rsend[PLANES - 1] = collect(PLANES - 1)
    r_copy(PLANES - 1).start()

    def mix(i, results):
        seen = lax.broadcasted_iota(jnp.int32, (tok, cap), 1).astype(jnp.float32)
        lane = lax.broadcasted_iota(jnp.int32, (tok, 2 * PLANES), 1)
        where = [jnp.sum(jnp.where(lane == 2 * i + k, pos_col[...], 0.0), axis=1, keepdims=True) for k in range(2)]
        first = (seen == where[0]).astype(jnp.float32).astype(jnp.bfloat16)
        second = (seen == where[1]).astype(jnp.float32).astype(jnp.bfloat16)
        mixed = gates[:, 0:1] * jnp.dot(first, results, preferred_element_type=jnp.float32)
        return mixed + gates[:, 1:2] * jnp.dot(second, results, preferred_element_type=jnp.float32)

    outacc[...] = jnp.zeros_like(outacc)

    def mix_body(i, carry):
        @pl.when(i > 0)
        def _():
            r_copy(i).wait_recv()

        outacc[...] += mix(i, rin[i])
        return carry

    lax.fori_loop(0, PLANES, mix_body, 0)
    out[...] = outacc[...].astype(jnp.bfloat16)

    for i in range(1, PLANES):
        y_copy(i).wait_send()
        meta_copy(i).wait_send()
        r_copy(i).wait_send()
    for i in range(PLANES):
        for j in range(1, SIDE):
            e_copy(i, j).wait_send()


def fused_moe(cap, x, pos_row, pos_col, gates, meta, w1, w3, w2):
    tok, model = x.shape
    rows = SIDE * BUCKET
    bf = jnp.bfloat16
    vmem = pl.BlockSpec(memory_space=pltpu.VMEM)
    hbm = pl.BlockSpec(memory_space=pl.ANY)
    dma = pltpu.SemaphoreType.DMA
    width = w1.shape[2]
    return pl.pallas_call(
        functools.partial(moe_kernel, cap),
        out_shape=jax.ShapeDtypeStruct((tok, model), bf),
        in_specs=[vmem] * 5 + [hbm] * 3,
        out_specs=vmem,
        scratch_shapes=[
            pltpu.VMEM((PLANES, cap, model), bf),
            pltpu.VMEM((PLANES - 1, cap, model), bf),
            pltpu.VMEM((PLANES, 2 * SIDE, rows), jnp.int32),
            pltpu.VMEM((PLANES, rows, model), bf),
            pltpu.VMEM((PLANES, rows, model), bf),
            pltpu.VMEM((PLANES, rows, model), bf),
            pltpu.VMEM((PLANES, cap, model), bf),
            pltpu.VMEM((PLANES, cap, model), bf),
            pltpu.VMEM((rows, model), jnp.float32),
            pltpu.VMEM((tok, model), jnp.float32),
            pltpu.VMEM((2, model, TILE), bf),
            pltpu.VMEM((2, model, TILE), bf),
            pltpu.VMEM((2, TILE, model), bf),
            dma((2, 3)),
            dma((PLANES,)),
            dma((PLANES,)),
            dma((PLANES,)),
            dma((PLANES,)),
            dma((PLANES, SIDE)),
            dma((PLANES, SIDE)),
            dma((PLANES, SIDE)),
            dma((PLANES, SIDE)),
            dma((PLANES,)),
            dma((PLANES,)),
        ],
        compiler_params=pltpu.CompilerParams(collective_id=0, has_side_effects=True, vmem_limit_bytes=67_000_000),
        cost_estimate=pl.CostEstimate(flops=6 * PLANES * rows * model * width, bytes_accessed=3 * PLANES * model * width * 2, transcendentals=0),
    )(x, pos_row, pos_col, gates, meta, w1, w3, w2)


def peak_kernel(n, mine, out, heard, ssem, rsem):
    me = lax.axis_index("ep")

    def copy(k):
        return pltpu.make_async_remote_copy(src_ref=mine, dst_ref=heard.at[k], send_sem=ssem.at[k], recv_sem=rsem.at[k], device_id=((me + k) % n,), device_id_type=MESH)

    barrier = pltpu.get_barrier_semaphore()
    for k in range(1, n):
        pl.semaphore_signal(barrier, inc=1, device_id=((me + k) % n,), device_id_type=MESH)
    pl.semaphore_wait(barrier, n - 1)
    for k in range(1, n):
        copy(k).start()
    heard[0] = mine[...]
    for k in range(1, n):
        copy(k).wait_recv()
    out[...] = jnp.max(heard[...], axis=0)
    for k in range(1, n):
        copy(k).wait_send()


def global_peak(n, most):
    vmem = pl.BlockSpec(memory_space=pltpu.VMEM)
    shape = (8, 128)
    peaks = pl.pallas_call(
        functools.partial(peak_kernel, n),
        out_shape=jax.ShapeDtypeStruct(shape, jnp.int32),
        in_specs=[vmem],
        out_specs=vmem,
        scratch_shapes=[pltpu.VMEM((n,) + shape, jnp.int32), pltpu.SemaphoreType.DMA((n,)), pltpu.SemaphoreType.DMA((n,))],
        compiler_params=pltpu.CompilerParams(collective_id=1, has_side_effects=True),
    )(jnp.full(shape, most, jnp.int32))
    return peaks[0, 0]


def route(hidden, w_router, ids, me):
    experts = w_router.shape[1]
    tok = ids.shape[0]
    plane, seat = me // SIDE, me % SIDE
    logits = jnp.dot(hidden.astype(jnp.float32), w_router, preferred_element_type=jnp.float32)
    probs = jax.nn.softmax(logits, axis=-1)
    chosen = [ids[:, k : k + 1] == jnp.arange(experts)[None, :] for k in range(2)]
    picked = [jnp.sum(jnp.where(c, probs, 0.0), axis=1, keepdims=True) for c in chosen]
    gates = jnp.concatenate(picked, axis=1) / (picked[0] + picked[1])
    named = chosen[0] | chosen[1]
    before = (jnp.arange(tok)[:, None] > jnp.arange(tok)[None, :]).astype(jnp.bfloat16)
    rank = (jnp.dot(before, named.astype(jnp.bfloat16), preferred_element_type=jnp.float32) + 0.5).astype(jnp.int32)
    counts = jnp.sum(named.astype(jnp.int32), axis=0)
    lane = jnp.arange(experts)
    start = jnp.sum(jnp.where(lane[None, :] < lane[:, None], counts[None, :], 0), axis=1)
    place = rank + start[None, :]
    pos = jnp.concatenate([jnp.sum(jnp.where(c, place, 0), axis=1, keepdims=True) for c in chosen], axis=1)
    planes = plane ^ jnp.arange(PLANES)
    plane_start = jnp.sum(jnp.where(lane[None, :] == planes[:, None] * SIDE, start[None, :], 0), axis=1)
    mine = (ids // SIDE)[:, None, :] == planes[None, :, None]
    pos_col = jnp.where(mine, pos[:, None, :] - plane_start[None, :, None], -1).reshape(tok, 2 * PLANES)
    dest = planes[:, None] * SIDE + (seat ^ jnp.arange(SIDE))[None, :]
    at_dest = dest[:, :, None] == lane[None, None, :]
    dest_start = jnp.sum(jnp.where(at_dest, start[None, None, :], 0), axis=2) - plane_start[:, None]
    dest_count = jnp.sum(jnp.where(at_dest, counts[None, None, :], 0), axis=2)
    slot = jnp.arange(BUCKET)
    home = jnp.where(slot[None, None, :] < dest_count[:, :, None], dest_start[:, :, None] + slot[None, None, :], -1)
    wide = SIDE * BUCKET
    meta = jnp.concatenate(
        [
            jnp.broadcast_to(dest_start[:, :, None], (PLANES, SIDE, wide)),
            jnp.broadcast_to(home.reshape(PLANES, 1, wide), (PLANES, SIDE, wide)),
        ],
        axis=1,
    )
    most = jnp.max(jnp.sum(counts.reshape(PLANES, SIDE), axis=1))
    return gates, pos_col.T.reshape(PLANES, 2, tok), pos_col.astype(jnp.float32), meta, most


CAPS = (304, 352, 512)


def solution(mesh):
    def device_body(hidden_loc, w_router, ids_loc, w_one, w_three, w_two):
        me = lax.axis_index("ep")
        gates, pos_row, pos_col, meta, most = route(hidden_loc, w_router, ids_loc, me)
        if len(CAPS) == 1:
            return fused_moe(CAPS[0], hidden_loc, pos_row, pos_col, gates, meta, w_one, w_three, w_two)
        gates, pos_row, pos_col, meta, most = lax.optimization_barrier((gates, pos_row, pos_col, meta, most))
        most = global_peak(mesh.shape["ep"], most)
        pick = sum((most > cap).astype(jnp.int32) for cap in CAPS[:-1])
        branches = [functools.partial(fused_moe, cap) for cap in CAPS]
        return lax.switch(pick, branches, hidden_loc, pos_row, pos_col, gates, meta, w_one, w_three, w_two)

    return jax.shard_map(device_body, mesh=mesh, in_specs=(P("ep", None), P(None, None), P("ep", None), P("ep", None, None), P("ep", None, None), P("ep", None, None)), out_specs=P("ep", None), check_vma=False)
```
